256 devices in a mesh: dp: 64 (over z, x, core), layer: 4 (over y).
Axes of the slice: x: 4, y: 4, z: 8, core: 2. Of those that a mesh axis runs over, the one named last changes fastest.
Arguments:
- acts: bfloat16 [4, 57344, 4608], P('layer', 'dp')
- probes: bfloat16 [4, 4608, 512], P('layer'), may hold values from -0.25 to 0.25
- labels: int32 [57344], P('dp'), may hold values from 0 to 511
Outputs:
- grads: float32 [4, 4608, 512], P('layer', 'dp')
- losses: float32 [4], P('layer')
The draws below stay inside these ranges and needn't reach their ends.
All inputs are finite; a program needn't handle non-finite values.
Results may differ from the reference program's by a relative error of at most 0.0013.
Values sent between devices are 32-bit elements; how exact they have to be, the bound alone decides.
A program may use at most 128 MiB of HBM per device.

```python
import jax
import jax.numpy as jnp
from jax import lax

D = 4608
C = 512
TOKENS = 57344
LAYERS = 4


def draw_acts(key, part):
    first = jax.random.fold_in(key, 0)
    base = jax.random.normal(first, (LAYERS, TOKENS, D), jnp.float32)
    base = jnp.clip(base, -6.0, 6.0)
    return base.astype(jnp.bfloat16)


def plant(entries, stream_key, low, high):
    extent = entries.shape
    spot = [jax.random.randint(jax.random.fold_in(stream_key, axis), (), 0, extent[axis]) for axis in range(len(extent))]
    entries = entries.at[tuple(spot)].set(low)
    longest = extent.index(max(extent))
    spot[longest] = (spot[longest] + 1) % extent[longest]
    return entries.at[tuple(spot)].set(high)


def levels(rng, shape, cuts, low, largest):
    level, own = 1.0, jax.random.fold_in(rng, 6)
    for dim, shards_of in cuts:
        steps = jnp.exp(jax.random.uniform(jax.random.fold_in(own, dim), (shards_of,), jnp.float32, low / len(cuts), largest / len(cuts)))
        level = level * jnp.repeat(steps, shape[dim] // shards_of).reshape([-1 if axis == dim else 1 for axis in range(len(shape))])
    return level


def noise(own_key, dims, scale, most, cuts=(), held_as=jnp.bfloat16):
    level = levels(own_key, dims, cuts, -0.22, 0.18) if cuts else 1.0
    array = jax.random.normal(own_key, dims, jnp.float32) * scale * level
    return jnp.minimum(jnp.maximum(array, -most), most).astype(held_as)


def setup_inputs(seed: int = 0) -> dict:
    seeds = jax.random.split(jax.random.key(seed), 4)
    return {
        "acts": draw_acts(jax.random.fold_in(seeds[3], 71), 0),
        "probes": noise(seeds[1], (LAYERS, D, C), (D // 9) ** -0.5, 0.25, ((0, 4),)),
        "labels": plant(jax.random.randint(seeds[2], (TOKENS,), 0, C), jax.random.fold_in(seeds[2], 1), 0, C - 1).astype(jnp.int32),
    }


def one_layer(item):
    acts_l, probe_l, onehot = item
    logits = jnp.dot(acts_l, probe_l, preferred_element_type=jnp.float32)
    top = jnp.max(logits, axis=1, keepdims=True)
    expo = jnp.exp(logits - top)
    total = jnp.sum(expo, axis=1, keepdims=True)
    probs = expo / total
    lse = top[:, 0] + jnp.log(total[:, 0])
    picked = jnp.sum(onehot * logits, axis=1)
    loss = jnp.sum(lse - picked) / jnp.float32(TOKENS)
    resid = (probs - onehot).astype(jnp.bfloat16)
    grad = lax.dot_general(acts_l, resid, (((0,), (0,)), ((), ())), preferred_element_type=jnp.float32)
    grad = grad * jnp.float32(1.0 / (TOKENS ** 0.5))
    return grad, loss


def reference(acts, probes, labels):
    classes = jnp.arange(C, dtype=jnp.int32)
    onehot = (labels[:, None] == classes[None, :]).astype(jnp.float32)

    def step(item):
        return one_layer((item[0], item[1], onehot))

    grads, losses = lax.map(step, (acts, probes))
    return grads, losses
```

```python
import jax
import jax.numpy as jnp
from jax import lax
from jax.experimental import pallas as pl
from jax.experimental.pallas import tpu as pltpu
from jax.sharding import PartitionSpec as P

F32 = jnp.float32
BF16 = jnp.bfloat16
MESH = pl.DeviceIdType.MESH

NX, NZ, NC = 4, 8, 2
SHARDS = NX * NZ * NC
ROWS = 8
TILE = 16
KSTEP = 512

WIDTHS = (256, 256, 384, 256, 256, 384, 256, 256, 384)
BEHIND = {2: 1, 3: 2, 4: 3, 5: 4, 6: 5, 7: 6}


def kernel(
    tokens, depth, classes, count_all,
    acts, probes, labels,
    grads, loss,
    a, w, at, acc, resid, lab,
    snd, own, r2, xa1, xa2, za1, za, zb1, zb, xb1, xb2,
    l1, l2, l3,
    load_sem, pair_send, pair_recv, send_sem, recv_sem, loss_send, loss_recv,
):
    dp = lax.axis_index("dp")
    core = lax.rem(dp, NC)
    chip = lax.div(dp, NC)
    x = lax.rem(chip, NX)
    z = lax.div(chip, NX)
    mate = 1 - core

    def at_x(step):
        return lax.rem(x + step + NX, NX)

    def at_z(step):
        return lax.rem(z + step + NZ, NZ)

    def device(zz, xx, cc):
        return {"dp": (zz * NX + xx) * NC + cc}

    pair = device(z, x, mate)
    along_x = [device(z, at_x(step), core) for step in range(1, NX)]
    along_z = [device(at_z(step), x, core) for step in range(1, NZ)]

    barrier = pltpu.get_barrier_semaphore()
    for peer in [pair] + along_x + along_z:
        pl.semaphore_signal(barrier, inc=1, device_id=peer, device_id_type=MESH)

    steps = depth // KSTEP
    tiles = KSTEP // TILE

    def loads(k):
        columns = pl.ds(k * KSTEP, KSTEP)
        return (
            pltpu.make_async_copy(probes.at[0, columns, :], w.at[k], load_sem.at[0, k]),
            pltpu.make_async_copy(acts.at[0, :, columns], a.at[k], load_sem.at[1, k]),
        )

    for k in range(steps):
        for load in loads(k):
            load.start()

    for block in range(tokens // 128):
        row = jnp.broadcast_to(labels[block : block + 1, :], (128, 128))
        lab[block * 128 : (block + 1) * 128, :] = row.T
    acc[...] = jnp.zeros_like(acc)

    @pl.loop(0, steps)
    def _(k):
        for load in (
            pltpu.make_async_copy(probes.at[0, pl.ds(0, KSTEP), :], w.at[k], load_sem.at[0, k]),
            pltpu.make_async_copy(acts.at[0, :, pl.ds(0, KSTEP)], a.at[k], load_sem.at[1, k]),
        ):
            load.wait()
        block = a[k]
        acc[...] += jnp.dot(block, w[k], preferred_element_type=F32)
        at[pl.ds(k * tiles, tiles)] = block.T.reshape(tiles, TILE, tokens)

    part = jnp.zeros((8, 128), F32)
    lane = lax.broadcasted_iota(jnp.int32, (128, 128), 1)
    names = lax.broadcasted_iota(jnp.int32, (128, classes), 1)
    for block in range(tokens // 128):
        rows = slice(block * 128, (block + 1) * 128)
        logits = acc[rows, :]
        hit = lab[rows, 0:1] == names
        top = jnp.max(logits, axis=1, keepdims=True)
        expo = jnp.exp(logits - top)
        total = jnp.sum(expo, axis=1, keepdims=True)
        lse = top + jnp.log(total)
        probs = expo * (1.0 / total)
        resid[rows, :] = jnp.where(hit, probs - 1.0, probs).astype(BF16)
        picked = jnp.where(hit, logits, 0.0)
        picked = sum(picked[:, 128 * i : 128 * (i + 1)] for i in range(classes // 128))
        each = jnp.where(lane == 0, lse, 0.0) - picked
        part = part + jnp.sum(each.reshape(16, 8, 128), axis=0)
    l1[core] = jnp.sum(part, axis=0, keepdims=True)

    pl.semaphore_wait(barrier, NC + NX + NZ - 3)

    def loss_copy(buf, mine, index, to, to_index):
        return pltpu.make_async_remote_copy(
            src_ref=buf.at[mine], dst_ref=buf.at[mine],
            send_sem=loss_send.at[index], recv_sem=loss_recv.at[to_index],
            device_id=to, device_id_type=MESH,
        )

    loss_stages = [
        [loss_copy(l1, core, 0, pair, 0)],
        [loss_copy(l2, x, i, along_x[i - 1], i) for i in range(1, NX)],
        [loss_copy(l3, z, NX + i - 1, along_z[i - 1], NX + i - 1) for i in range(1, NZ)],
    ]

    def loss_stage(step):
        if step > 0:
            for copy in loss_stages[step - 1]:
                copy.wait_recv()
            if step == 1:
                l2[x] = l1[0] + l1[1]
            elif step == 2:
                l3[z] = (l2[0] + l2[1]) + (l2[2] + l2[3])
            else:
                rows = [l3[i] for i in range(NZ)]
                while len(rows) > 1:
                    rows = [p + q for p, q in zip(rows[::2], rows[1::2])]
                whole = jnp.sum(rows[0], axis=1, keepdims=True) / F32(count_all)
                loss[...] = jnp.broadcast_to(whole, (1, 128))
        if step < 3:
            for copy in loss_stages[step]:
                copy.start()

    def terms(tile):
        lhs = jnp.concatenate([at[i * 9 + tile] for i in range(NX * NZ)], axis=0)
        out = jnp.dot(lhs, resid[...], preferred_element_type=F32)
        return out.reshape(NX * NZ, 2, ROWS, classes)

    def store(buf, chunk, value):
        buf[chunk] = value.reshape(NZ, NX, ROWS, classes)

    def pair_copy(i):
        return pltpu.make_async_remote_copy(
            src_ref=snd.at[i], dst_ref=r2.at[i],
            send_sem=pair_send.at[i], recv_sem=pair_recv.at[i],
            device_id=pair, device_id_type=MESH,
        )

    pair_copies = [pair_copy(i) for i in range(9)]

    def terms_for_pair(k):
        both = terms(k + 5 * mate)
        for half in range(2):
            store(snd, 2 * k + half, both[:, half])
            pair_copies[2 * k + half].start()

    def terms_for_own(k):
        both = terms(k + 5 * core)
        for half in range(2):
            store(own, 2 * k + half, both[:, half])

    def terms_for_both():
        both = terms(4)
        first = core == 0
        store(snd, 8, jnp.where(first, both[:, 1], both[:, 0]))
        pair_copies[8].start()
        store(own, 8, jnp.where(first, both[:, 0], both[:, 1]))

    sent = {}
    xs = {step: at_x(step) for step in (-1, 1, 2)}
    zs = {step: at_z(step) for step in (-3, -2, -1, 1, 2, 3, 4)}
    to_x = {1: along_x[0], -1: along_x[NX - 2]}
    to_z = {1: along_z[0], -1: along_z[NZ - 2]}
    SIDE = {1: 0, -1: 1}

    def send(i, name, d, src, dst, to):
        slot = SLOTS.index((name, d))
        copy = pltpu.make_async_remote_copy(
            src_ref=src, dst_ref=dst,
            send_sem=send_sem.at[i, slot], recv_sem=recv_sem.at[i, slot],
            device_id=to, device_id_type=MESH,
        )
        copy.start()
        sent[i, name, d] = copy

    def arrived(i, name, d):
        sent[i, name, d].wait_recv()

    def stage(i, step):
        wa = WIDTHS[i]
        ca, cb = pl.ds(0, wa), pl.ds(wa, classes - wa)
        far = 1 if i % 2 == 0 else -1
        halves_z = {1: pl.ds(0, NZ // 2), -1: pl.ds(NZ // 2, NZ // 2)}
        halves_x = {1: pl.ds(0, NX // 2), -1: pl.ds(NX // 2, NX // 2)}
        if step == 1:
            pair_copies[i].wait_recv()
            own[i] += r2[i]
            for d in (1, -1):
                send(i, "xa1", d, own.at[i, halves_z[d], xs[2], :, ca], xa1.at[i, SIDE[d], :, :, ca], to_x[d])
                send(i, "zb1", d, own.at[i, zs[4], halves_x[d], :, cb], zb1.at[i, SIDE[d], :, :, cb], to_z[d])
        elif step == 2:
            for d in (1, -1):
                arrived(i, "xa1", d)
                own[i, halves_z[d], xs[d], :, ca] += xa1[i, SIDE[d], :, :, ca]
            for d in (1, -1):
                send(i, "xa2", d, own.at[i, :, xs[d], :, ca], xa2.at[i, SIDE[d], :, :, ca], to_x[d])
            for d in (1, -1):
                arrived(i, "zb1", d)
                own[i, zs[3 * d], halves_x[d], :, cb] += zb1[i, SIDE[d], :, :, cb]
            for d in (1, -1):
                send(i, "zb2", d, own.at[i, zs[3 * d], :, :, cb], zb.at[i, 0, SIDE[d], :, :, cb], to_z[d])
        elif step == 3:
            for d in (1, -1):
                arrived(i, "xa2", d)
            own[i, :, x, :, ca] += xa2[i, 0, :, :, ca] + xa2[i, 1, :, :, ca]
            send(i, "za1", far, own.at[i, zs[4], x, :, ca], za1.at[i, :, ca], to_z[far])
            for d in (1, -1):
                arrived(i, "zb2", d)
                own[i, zs[2 * d], :, :, cb] += zb[i, 0, SIDE[d], :, :, cb]
                send(i, "zb3", d, own.at[i, zs[2 * d], :, :, cb], zb.at[i, 1, SIDE[d], :, :, cb], to_z[d])
        elif step == 4:
            arrived(i, "za1", far)
            own[i, zs[3 * far], x, :, ca] += za1[i, :, ca]
            for d in (1, -1):
                send(i, "za2", d, own.at[i, zs[3 * d], x, :, ca], za.at[i, 0, SIDE[d], :, ca], to_z[d])
            for d in (1, -1):
                arrived(i, "zb3", d)
                own[i, zs[d], :, :, cb] += zb[i, 1, SIDE[d], :, :, cb]
                send(i, "zb4", d, own.at[i, zs[d], :, :, cb], zb.at[i, 2, SIDE[d], :, :, cb], to_z[d])
        elif step == 5:
            for d in (1, -1):
                arrived(i, "za2", d)
                own[i, zs[2 * d], x, :, ca] += za[i, 0, SIDE[d], :, ca]
                send(i, "za3", d, own.at[i, zs[2 * d], x, :, ca], za.at[i, 1, SIDE[d], :, ca], to_z[d])
            for d in (1, -1):
                arrived(i, "zb4", d)
            own[i, z, :, :, cb] += zb[i, 2, 0, :, :, cb] + zb[i, 2, 1, :, :, cb]
            send(i, "xb1", far, own.at[i, z, xs[2], :, cb], xb1.at[i, :, cb], to_x[far])
        elif step == 6:
            for d in (1, -1):
                arrived(i, "za3", d)
                own[i, zs[d], x, :, ca] += za[i, 1, SIDE[d], :, ca]
                send(i, "za4", d, own.at[i, zs[d], x, :, ca], za.at[i, 2, SIDE[d], :, ca], to_z[d])
            arrived(i, "xb1", far)
            own[i, z, xs[far], :, cb] += xb1[i, :, cb]
            for d in (1, -1):
                send(i, "xb2", d, own.at[i, z, xs[d], :, cb], xb2.at[i, SIDE[d], :, cb], to_x[d])
        else:
            row = i * ROWS + core * ROWS if i < 8 else mate * (8 * ROWS)
            rows = pl.ds(pl.multiple_of(row, ROWS), ROWS)
            factor = F32(1.0 / count_all**0.5)
            for d in (1, -1):
                arrived(i, "za4", d)
            grads[rows, ca] = (own[i, z, x, :, ca] + (za[i, 2, 0, :, ca] + za[i, 2, 1, :, ca])) * factor
            for d in (1, -1):
                arrived(i, "xb2", d)
            grads[rows, cb] = (own[i, z, x, :, cb] + (xb2[i, 0, :, cb] + xb2[i, 1, :, cb])) * factor

    loss_stage(0)
    computes = [
        [lambda: terms_for_pair(0), lambda: terms_for_own(0), lambda: terms_for_pair(1)],
        [lambda: terms_for_own(1), lambda: terms_for_pair(2)],
        [lambda: terms_for_own(2), lambda: terms_for_pair(3)],
        [lambda: terms_for_own(3), terms_for_both],
    ]
    chunks = 9
    for slot in range(chunks + max(BEHIND.values())):
        if slot < len(computes):
            for compute in computes[slot]:
                compute()
        for step in range(1, 8):
            i = slot - BEHIND.get(step, 0)
            if 0 <= i < chunks:
                stage(i, step)
        if slot in (1, 3, 6):
            loss_stage({1: 1, 3: 2, 6: 3}[slot])

    for copy in pair_copies:
        copy.wait_send()
    for group in loss_stages:
        for copy in group:
            copy.wait_send()
    for copy in sent.values():
        copy.wait_send()


SLOTS = [
    (name, d)
    for name in ("xa1", "xa2", "za2", "za3", "za4", "zb1", "zb2", "zb3", "zb4", "xb2")
    for d in (1, -1)
]
SLOTS += [("za1", 1), ("za1", -1), ("xb1", 1), ("xb1", -1)]


def per_device(acts, probes, labels):
    tokens, depth = acts.shape[1:]
    classes = probes.shape[2]
    count_all = tokens * SHARDS
    n = depth // SHARDS // ROWS
    steps = depth // KSTEP
    vmem, sems = pltpu.VMEM, pltpu.SemaphoreType.DMA
    grads, loss = pl.pallas_call(
        lambda *refs: kernel(tokens, depth, classes, count_all, *refs),
        out_shape=(
            jax.ShapeDtypeStruct((depth // SHARDS, classes), F32),
            jax.ShapeDtypeStruct((1, 128), F32),
        ),
        in_specs=[
            pl.BlockSpec(memory_space=pl.ANY),
            pl.BlockSpec(memory_space=pl.ANY),
            pl.BlockSpec(memory_space=pltpu.VMEM),
        ],
        out_specs=(pl.BlockSpec(memory_space=pltpu.VMEM),) * 2,
        scratch_shapes=[
            vmem((steps, tokens, KSTEP), BF16),
            vmem((steps, KSTEP, classes), BF16),
            vmem((depth // TILE, TILE, tokens), BF16),
            vmem((tokens, classes), F32),
            vmem((tokens, classes), BF16),
            vmem((tokens, 128), jnp.int32),
            vmem((n, NZ, NX, ROWS, classes), F32),
            vmem((n, NZ, NX, ROWS, classes), F32),
            vmem((n, NZ, NX, ROWS, classes), F32),
            vmem((n, 2, NZ // 2, ROWS, classes), F32),
            vmem((n, 2, NZ, ROWS, classes), F32),
            vmem((n, ROWS, classes), F32),
            vmem((n, 3, 2, ROWS, classes), F32),
            vmem((n, 2, NX // 2, ROWS, classes), F32),
            vmem((n, 3, 2, NX, ROWS, classes), F32),
            vmem((n, ROWS, classes), F32),
            vmem((n, 2, ROWS, classes), F32),
            vmem((NC, 1, 128), F32),
            vmem((NX, 1, 128), F32),
            vmem((NZ, 1, 128), F32),
            sems((2, steps)),
            sems((n,)),
            sems((n,)),
            sems((n, len(SLOTS))),
            sems((n, len(SLOTS))),
            sems((NX + NZ - 1,)),
            sems((NX + NZ - 1,)),
        ],
        compiler_params=pltpu.CompilerParams(
            collective_id=0, has_side_effects=True, vmem_limit_bytes=62 * 1024 * 1024
        ),
        name="probe_step",
    )(acts, probes, labels.reshape(tokens // 128, 128))
    return grads[None], loss[0, :1]


def solution(mesh):
    return jax.shard_map(
        per_device,
        mesh=mesh,
        in_specs=(P("layer", "dp", None), P("layer", None, None), P("dp")),
        out_specs=(P("layer", "dp", None), P("layer")),
        check_vma=False,
    )
```

```python
import jax
import jax.numpy as jnp
from jax import lax
from jax.experimental import pallas as pl
from jax.experimental.pallas import tpu as pltpu
from jax.sharding import PartitionSpec as P

F32 = jnp.float32
BF16 = jnp.bfloat16
MESH = pl.DeviceIdType.MESH

NX, NZ, NC = 4, 8, 2
SHARDS = NX * NZ * NC
ROWS = 8
TILE = 16
KSTEP = 768
AHEAD = 2

WIDTHS = (256, 256, 384, 256, 256, 384, 256, 256, 384)
STEPS = {
    "x1": [[(2, 2), (1, 1)]],
    "x2": [[(2, 1)], [(1, 1)]],
    "z2": [[(4, 2), (3, 1)], [(2, 2), (1, 1)]],
    "z4": [[(4, 1)], [(3, 1)], [(2, 1)], [(1, 1)]],
}
PLANS = (
    ("x2", "z2", "z4", "x1"),
    ("x2", "z2", "z4", "x1"),
    ("x2", "z2", "z4", "x1"),
    ("x2", "z2", "z4", "x1"),
    ("x2", "z2", "z4", "x1"),
    ("x2", "z2", "z4", "x1"),
    ("x2", "z2", "z4", "x1"),
    ("x2", "z2", "z4", "x1"),
    ("x2", "z2", "z4", "x1"),
)
ORDER = (
    (0, 0, 0), (1, 0, 0), (0, 1, 0), (1, 1, 0), (5, 0, 0), (0, 2, 0), (3, 0, 0), (4, 0, 0),
    (1, 2, 0), (3, 1, 0), (4, 1, 0), (0, 3, 0), (1, 3, 0), (3, 2, 0), (4, 2, 0), (2, 0, 0),
    (5, 0, 1), (3, 3, 0), (4, 3, 0), (4, 0, 1), (3, 4, 0), (4, 4, 0), (3, 0, 1), (4, 1, 1),
    (3, 1, 1), (3, 5, 0), (4, 5, 0), (4, 2, 1), (3, 6, 0), (4, 6, 0), (3, 2, 1), (4, 3, 1),
    (3, 7, 0), (4, 7, 0), (3, 3, 1), (4, 0, 2), (3, 8, 0), (4, 4, 1), (3, 4, 1), (4, 8, 0),
    (4, 1, 2), (4, 5, 1), (4, 2, 2), (3, 0, 2), (4, 6, 1), (5, 0, 2), (4, 3, 2), (4, 7, 1),
    (3, 1, 2), (4, 0, 3), (3, 5, 1), (4, 4, 2), (4, 8, 1), (3, 6, 1), (4, 1, 3), (4, 5, 2),
    (4, 2, 3), (3, 0, 3), (3, 2, 2), (4, 6, 2), (3, 7, 1), (4, 3, 3), (4, 7, 2), (3, 1, 3),
    (3, 3, 2), (4, 0, 4), (5, 0, 3), (4, 4, 3), (3, 8, 1), (4, 8, 2), (4, 1, 4), (4, 5, 3),
    (3, 4, 2), (4, 2, 4), (3, 0, 4), (3, 2, 3), (3, 5, 2), (4, 6, 3), (4, 3, 4), (3, 6, 2),
    (4, 7, 3), (3, 1, 4), (3, 3, 3), (3, 7, 2), (4, 4, 4), (4, 8, 3), (4, 0, 5), (4, 5, 4),
    (3, 4, 3), (3, 2, 4), (3, 8, 2), (3, 5, 3), (4, 1, 5), (4, 6, 4), (4, 2, 5), (4, 3, 5),
    (3, 6, 3), (4, 4, 5), (4, 7, 4), (4, 5, 5), (3, 3, 4), (3, 7, 3), (4, 8, 4), (3, 4, 4),
    (3, 8, 3), (4, 6, 5), (3, 5, 4), (4, 7, 5), (3, 6, 4), (4, 8, 5), (3, 7, 4), (3, 8, 4),
)


def kernel(
    tokens, depth, classes, count_all,
    acts, probes, labels,
    grads, loss,
    a, w, at, acc, resid, lab, raw,
    snd, own, r2, xa2, xa1, za, zb4, zb, xb,
    l1, l2, l3, gauge, row_gauge,
    load_sem, label_sem, pair_send, pair_recv, send_sem, recv_sem, loss_send, loss_recv,
):
    dp = lax.axis_index("dp")
    core = lax.rem(dp, NC)
    chip = lax.div(dp, NC)
    x = lax.rem(chip, NX)
    z = lax.div(chip, NX)
    mate = 1 - core

    def at_x(step):
        return lax.rem(x + step + NX, NX)

    def at_z(step):
        return lax.rem(z + step + NZ, NZ)

    def device(zz, xx, cc):
        return {"dp": (zz * NX + xx) * NC + cc}

    pair = device(z, x, mate)
    along_x = [device(z, at_x(step), core) for step in range(1, NX)]
    along_z = [device(at_z(step), x, core) for step in range(1, NZ)]

    barrier = pltpu.get_barrier_semaphore()
    for peer in [pair] + along_x + along_z:
        pl.semaphore_signal(barrier, inc=1, device_id=peer, device_id_type=MESH)

    steps = depth // KSTEP
    tiles = KSTEP // TILE

    def loads(k):
        columns = pl.ds(pl.multiple_of(k * KSTEP, KSTEP), KSTEP)
        return (
            pltpu.make_async_copy(probes.at[0, columns, :], w.at[k], load_sem.at[0, k]),
            pltpu.make_async_copy(acts.at[0, :, columns], a.at[k], load_sem.at[1, k]),
        )

    for k in range(AHEAD):
        for load in loads(k):
            load.start()
    label_load = pltpu.make_async_copy(labels, raw, label_sem)
    label_load.start()

    acc[...] = jnp.zeros_like(acc)

    @pl.loop(0, steps)
    def _(k):
        for load in loads(k):
            load.wait()

        @pl.when(k + AHEAD < steps)
        def _():
            for load in loads(k + AHEAD):
                load.start()

        block = a[k]
        acc[...] += jnp.dot(block, w[k], preferred_element_type=F32)
        at[pl.ds(k * tiles, tiles)] = block.T.reshape(tiles, TILE, tokens)

    label_load.wait()
    for block in range(tokens // 128):
        row = jnp.broadcast_to(raw[block : block + 1, :], (128, 128))
        lab[block * 128 : (block + 1) * 128, :] = row.T
    part = jnp.zeros((8, 128), F32)
    lane = lax.broadcasted_iota(jnp.int32, (128, 128), 1)
    names = lax.broadcasted_iota(jnp.int32, (128, classes), 1)
    for block in range(tokens // 128):
        rows = slice(block * 128, (block + 1) * 128)
        logits = acc[rows, :]
        hit = lab[rows, 0:1] == names
        top = jnp.max(logits, axis=1, keepdims=True)
        expo = jnp.exp(logits - top)
        total = jnp.sum(expo, axis=1, keepdims=True)
        lse = top + jnp.log(total)
        probs = expo * (1.0 / total)
        resid[rows, :] = jnp.where(hit, probs - 1.0, probs).astype(BF16)
        picked = jnp.where(hit, logits, 0.0)
        picked = sum(picked[:, 128 * i : 128 * (i + 1)] for i in range(classes // 128))
        each = jnp.where(lane == 0, lse, 0.0) - picked
        part = part + jnp.sum(each.reshape(16, 8, 128), axis=0)
    l1[core] = jnp.sum(part, axis=0, keepdims=True)

    pl.semaphore_wait(barrier, NC + NX + NZ - 3)

    def whole_of(buf, count, sent_sem, got_sem):
        part = buf.at[pl.ds(0, count)]
        return pltpu.make_async_remote_copy(
            src_ref=part, dst_ref=part, send_sem=sent_sem, recv_sem=got_sem,
            device_id=pair, device_id_type=MESH,
        )

    def loss_copy(buf, mine, stage_index, to):
        return pltpu.make_async_remote_copy(
            src_ref=buf.at[mine], dst_ref=buf.at[mine],
            send_sem=loss_send, recv_sem=loss_recv.at[stage_index],
            device_id=to, device_id_type=MESH,
        )

    loss_stages = [
        [loss_copy(l1, core, 0, pair)],
        [loss_copy(l2, x, 1, to) for to in along_x],
        [loss_copy(l3, z, 2, to) for to in along_z],
    ]

    def loss_stage(step):
        if step > 0:
            whole_of(row_gauge, len(loss_stages[step - 1]), loss_send, loss_recv.at[step - 1]).wait_recv()
            if step == 1:
                l2[x] = l1[0] + l1[1]
            elif step == 2:
                l3[z] = (l2[0] + l2[1]) + (l2[2] + l2[3])
            else:
                rows = [l3[i] for i in range(NZ)]
                while len(rows) > 1:
                    rows = [p + q for p, q in zip(rows[::2], rows[1::2])]
                whole = jnp.sum(rows[0], axis=1, keepdims=True) / F32(count_all)
                loss[...] = jnp.broadcast_to(whole, (1, 128))
        if step < 3:
            for copy in loss_stages[step]:
                copy.start()

    def terms(tile):
        lhs = jnp.concatenate([at[i * 9 + tile] for i in range(NX * NZ)], axis=0)
        out = jnp.dot(lhs, resid[...], preferred_element_type=F32)
        return out.reshape(NX * NZ, 2, ROWS, classes)

    def store(buf, chunk, value):
        buf[chunk] = value.reshape(NZ, NX, ROWS, classes)

    def pair_copy(i):
        return pltpu.make_async_remote_copy(
            src_ref=snd.at[i], dst_ref=r2.at[i],
            send_sem=pair_send, recv_sem=pair_recv.at[i],
            device_id=pair, device_id_type=MESH,
        )

    pair_copies = [pair_copy(i) for i in range(9)]

    def terms_for_pair(k):
        both = terms(k + 5 * mate)
        for half in range(2):
            store(snd, 2 * k + half, both[:, half])
            pair_copies[2 * k + half].start()

    def terms_for_own(k):
        both = terms(k + 5 * core)
        for half in range(2):
            store(own, 2 * k + half, both[:, half])

    def terms_for_both():
        both = terms(4)
        first = core == 0
        store(snd, 8, jnp.where(first, both[:, 1], both[:, 0]))
        pair_copies[8].start()
        store(own, 8, jnp.where(first, both[:, 0], both[:, 1]))

    ring = {"x": (at_x, along_x, NX), "z": (at_z, along_z, NZ)}
    counts = []

    def size(i, stream, which, j):
        lanes = (WIDTHS[i] if stream == 0 else classes - WIDTHS[i]) // 128
        if which == 1:
            return lanes
        lanes *= NZ if stream == 0 else NX
        return lanes // 2 if j == (NX if stream == 0 else NZ) // 2 else lanes

    def slot(stream, step):
        return stream * MOST + step

    def parts(i, stream):
        wa = WIDTHS[i]
        plan = PLANS[i]
        if stream == 0:
            cols = pl.ds(0, wa)
            half = {1: pl.ds(0, NZ // 2), -1: pl.ds(NZ // 2, NZ // 2)}

            def first(j, d):
                if j == NX // 2:
                    side = (half[d], at_x(j * d), slice(None), cols)
                else:
                    side = (slice(None), at_x(j * d), slice(None), cols)
                return (i,) + side

            def first_land(j, d):
                if j == NX // 2:
                    return xa2, (i, SIDE[d], slice(None), slice(None), cols)
                return xa1, (i, SIDE[d], slice(None), slice(None), cols)

            def after(j, d, k):
                kept = half[d] if j == NX // 2 else slice(None)
                return (i, kept, at_x(k * d), slice(None), cols)

            def second(j, d):
                return (i, at_z(j * d), x, slice(None), cols)

            def second_land(j, d):
                return za, (i, j - 1, SIDE[d], slice(None), cols)

            return ("x", plan[0], first, first_land, after), ("z", plan[1], second, second_land, None)
        cols = pl.ds(wa, classes - wa)
        half = {1: pl.ds(0, NX // 2), -1: pl.ds(NX // 2, NX // 2)}

        def first(j, d):
            kept = half[d] if j == NZ // 2 else slice(None)
            return (i, at_z(j * d), kept, slice(None), cols)

        def first_land(j, d):
            if j == NZ // 2:
                return zb4, (i, SIDE[d], slice(None), slice(None), cols)
            return zb, (i, j - 1, SIDE[d], slice(None), slice(None), cols)

        def after(j, d, k):
            kept = half[d] if j == NZ // 2 else slice(None)
            return (i, at_z(k * d), kept, slice(None), cols)

        def second(j, d):
            return (i, z, at_x(j * d), slice(None), cols)

        def second_land(j, d):
            return xb, (i, j - 1, SIDE[d], slice(None), cols)

        return ("z", plan[2], first, first_land, after), ("x", plan[3], second, second_land, None)

    def moves(i, phase, big):
        far = 1 if i % 2 == 0 else -1
        axis, steps = phase[0], STEPS[phase[1]]
        top = ring[axis][2] // 2
        return [
            [(j, h, d) for j, h in step for d in (1, -1) if big or j < top or d == far]
            for step in steps
        ]

    def stage(i, stream, step):
        phases = parts(i, stream)
        todo = [(0, m) for m in moves(i, phases[0], True)] + [(1, m) for m in moves(i, phases[1], False)]
        if step == 0 and ready.setdefault(i, True):
            pair_copies[i].wait_recv()
            own[i] += r2[i]
            ready[i] = False
        if step > 0:
            which, group = todo[step - 1]
            axis, _, place, land, after = phases[which]
            finals = []
            count = sum(size(i, stream, which, j) for j, h, d in group)
            whole_of(gauge, count, send_sem, recv_sem.at[i, slot(stream, step - 1)]).wait_recv()
            for j, h, d in group:
                buf, index = land(j, d)
                if j == h:
                    finals.append((buf, index, j, d))
                else:
                    spot = after(j, d, j - h) if after else place(j - h, d)
                    own[spot] += buf[index]
            last.setdefault((i, stream, which), []).extend(finals)
            if step == len(todo) or todo[step][0] != which:
                finals = last[i, stream, which]
                top = ring[axis][2] // 2
                if which == 0:
                    whole = [buf[index] for buf, index, j, d in finals if j < top]
                    spot = place(0, 1)
                    total = own[spot]
                    for value in whole:
                        total += value
                    own[spot] = total
                    for buf, index, j, d in finals:
                        if j == top:
                            own[after(j, d, 0)] += buf[index]
                else:
                    total = own[place(0, 1)]
                    for buf, index, j, d in finals:
                        total += buf[index]
                    row = i * ROWS + core * ROWS if i < 8 else mate * (8 * ROWS)
                    rows = pl.ds(pl.multiple_of(row, ROWS), ROWS)
                    grads[rows, index[-1]] = total * F32(1.0 / count_all**0.5)
        if step < len(todo):
            which, group = todo[step]
            axis, _, place, land, _ = phases[which]
            _, peers, _ = ring[axis]
            for j, h, d in group:
                buf, index = land(j, d)
                copy = pltpu.make_async_remote_copy(
                    src_ref=own.at[place(j, d)], dst_ref=buf.at[index],
                    send_sem=send_sem, recv_sem=recv_sem.at[i, slot(stream, step)],
                    device_id=peers[h - 1 if d > 0 else len(peers) - h], device_id_type=MESH,
                )
                copy.start()
                counts.append(size(i, stream, which, j))

    SIDE = {1: 0, -1: 1}
    ready, last = {}, {}
    for code, i, step in ORDER:
        if code == 0:
            terms_for_pair(i)
        elif code == 1:
            terms_for_own(i)
        elif code == 2:
            terms_for_both()
        elif code == 5:
            loss_stage(step)
        else:
            stage(i, code - 3, step)

    pltpu.make_async_remote_copy(
        src_ref=snd, dst_ref=r2, send_sem=pair_send, recv_sem=pair_recv.at[0],
        device_id=pair, device_id_type=MESH,
    ).wait_send()
    whole_of(row_gauge, sum(len(group) for group in loss_stages), loss_send, loss_recv.at[0]).wait_send()
    assert sum(counts) == copied_tiles(classes)
    whole_of(gauge, sum(counts), send_sem, recv_sem.at[0, 0]).wait_send()


def copied_tiles(classes):
    total = 0
    for width, plan in zip(WIDTHS, PLANS):
        for lanes, first, second, n, m in (
            (width // 128, plan[0], plan[1], NX, NZ),
            ((classes - width) // 128, plan[2], plan[3], NZ, NX),
        ):
            for steps in STEPS[first]:
                total += sum(lanes * m * (1 if j == n // 2 else 2) for j, h in steps)
            for steps in STEPS[second]:
                total += sum(lanes * (1 if j == m // 2 else 2) for j, h in steps)
    return total


MOST = 5


def per_device(acts, probes, labels):
    tokens, depth = acts.shape[1:]
    classes = probes.shape[2]
    count_all = tokens * SHARDS
    n = depth // SHARDS // ROWS
    steps = depth // KSTEP
    vmem, sems = pltpu.VMEM, pltpu.SemaphoreType.DMA
    grads, loss = pl.pallas_call(
        lambda *refs: kernel(tokens, depth, classes, count_all, *refs),
        out_shape=(
            jax.ShapeDtypeStruct((depth // SHARDS, classes), F32),
            jax.ShapeDtypeStruct((1, 128), F32),
        ),
        in_specs=[
            pl.BlockSpec(memory_space=pl.ANY),
            pl.BlockSpec(memory_space=pl.ANY),
            pl.BlockSpec(memory_space=pl.ANY),
        ],
        out_specs=(pl.BlockSpec(memory_space=pltpu.VMEM),) * 2,
        scratch_shapes=[
            vmem((steps, tokens, KSTEP), BF16),
            vmem((steps, KSTEP, classes), BF16),
            vmem((depth // TILE, TILE, tokens), BF16),
            vmem((tokens, classes), F32),
            vmem((tokens, classes), BF16),
            vmem((tokens, 128), jnp.int32),
            vmem((tokens // 128, 128), jnp.int32),
            vmem((n, NZ, NX, ROWS, classes), F32),
            vmem((n, NZ, NX, ROWS, classes), F32),
            vmem((n, NZ, NX, ROWS, classes), F32),
            vmem((n, 2, NZ // 2, ROWS, classes), F32),
            vmem((n, 2, NZ, ROWS, classes), F32),
            vmem((n, 4, 2, ROWS, classes), F32),
            vmem((n, 2, NX // 2, ROWS, classes), F32),
            vmem((n, 3, 2, NX, ROWS, classes), F32),
            vmem((n, 2, 2, ROWS, classes), F32),
            vmem((NC, 1, 128), F32),
            vmem((NX, 1, 128), F32),
            vmem((NZ, 1, 128), F32),
            vmem((copied_tiles(classes), 8, 128), F32),
            vmem((16, 1, 128), F32),
            sems((2, steps)),
            sems(()),
            sems(()),
            sems((n,)),
            sems(()),
            sems((n, 2 * MOST)),
            sems(()),
            sems((3,)),
        ],
        compiler_params=pltpu.CompilerParams(
            collective_id=0, has_side_effects=True, vmem_limit_bytes=62 * 1024 * 1024
        ),
        name="probe_step",
    )(acts, probes, labels.reshape(tokens // 128, 128))
    return grads[None], loss[0, :1]


def solution(mesh):
    return jax.shard_map(
        per_device,
        mesh=mesh,
        in_specs=(P("layer", "dp", None), P("layer", None, None), P("dp")),
        out_specs=(P("layer", "dp", None), P("layer")),
        check_vma=False,
    )
```

```python
import jax
import jax.numpy as jnp
from jax import lax
from jax.experimental import pallas as pl
from jax.experimental.pallas import tpu as pltpu
from jax.sharding import PartitionSpec as P

F32 = jnp.float32
BF16 = jnp.bfloat16
MESH = pl.DeviceIdType.MESH

NX, NZ, NC = 4, 8, 2
SHARDS = NX * NZ * NC
ROWS = 8
TILE = 16
KSTEP = 768
AHEAD = 2

WIDTHS = (128, 256, 256, 384, 384, 384, 128, 384, 256)
STEPS = {
    "x1": [[(2, 2), (1, 1)]],
    "x2": [[(2, 1)], [(1, 1)]],
    "z1": [[(4, 4), (3, 3), (2, 2), (1, 1)]],
    "z2": [[(4, 2), (3, 1)], [(2, 2), (1, 1)]],
    "z3": [[(4, 2), (3, 1)], [(2, 1)], [(1, 1)]],
    "z4": [[(4, 1)], [(3, 1)], [(2, 1)], [(1, 1)]],
}
PLANS = (
    ("x1", "z3", "z4", "x1"),
    ("x2", "z4", "z3", "x2"),
    ("x2", "z4", "z3", "x2"),
    ("x2", "z4", "z4", "x2"),
    ("x2", "z3", "z4", "x1"),
    ("x2", "z3", "z2", "x2"),
    ("x2", "z2", "z4", "x1"),
    ("x2", "z2", "z4", "x2"),
    ("x2", "z1", "z4", "x1"),
)
ORDER = (
    (0, 0, 0), (1, 0, 0), (0, 1, 0), (1, 1, 0), (5, 0, 0), (0, 2, 0), (3, 0, 0), (4, 0, 0),
    (1, 2, 0), (3, 1, 0), (4, 1, 0), (0, 3, 0), (1, 3, 0), (3, 2, 0), (4, 2, 0), (2, 0, 0),
    (5, 0, 1), (3, 3, 0), (4, 3, 0), (3, 4, 0), (4, 4, 0), (4, 0, 1), (3, 5, 0), (4, 5, 0),
    (3, 0, 1), (3, 1, 1), (4, 1, 1), (3, 6, 0), (4, 6, 0), (3, 2, 1), (3, 7, 0), (4, 7, 0),
    (4, 2, 1), (4, 3, 1), (3, 3, 1), (4, 4, 1), (3, 8, 0), (4, 8, 0), (3, 4, 1), (4, 0, 2),
    (5, 0, 2), (4, 5, 1), (3, 5, 1), (3, 0, 2), (4, 1, 2), (4, 6, 1), (4, 7, 1), (3, 1, 2),
    (3, 6, 1), (4, 2, 2), (4, 3, 2), (4, 4, 2), (4, 8, 1), (3, 2, 2), (4, 0, 3), (3, 7, 1),
    (4, 5, 2), (3, 0, 3), (4, 1, 3), (3, 3, 2), (5, 0, 3), (3, 8, 1), (4, 6, 2), (4, 7, 2),
    (3, 1, 3), (4, 2, 3), (4, 3, 3), (4, 4, 3), (3, 4, 2), (4, 8, 2), (3, 2, 3), (4, 0, 4),
    (3, 0, 4), (3, 3, 3), (3, 5, 2), (3, 6, 2), (4, 6, 3), (4, 7, 3), (3, 1, 4), (4, 3, 4),
    (4, 4, 4), (3, 4, 3), (3, 7, 2), (4, 5, 3), (4, 1, 4), (4, 8, 3), (3, 2, 4), (3, 3, 4),
    (3, 5, 3), (4, 2, 4), (3, 8, 2), (3, 6, 3), (4, 3, 5), (4, 0, 5), (4, 6, 4), (4, 7, 4),
    (4, 5, 4), (3, 1, 5), (4, 4, 5), (4, 1, 5), (3, 4, 4), (3, 7, 3), (4, 2, 5), (4, 8, 4),
    (3, 2, 5), (4, 3, 6), (3, 3, 5), (3, 5, 4), (4, 7, 5), (4, 6, 5), (3, 8, 3), (3, 1, 6),
    (3, 4, 5), (3, 6, 4), (3, 7, 4), (3, 2, 6), (4, 8, 5), (3, 3, 6), (4, 7, 6), (3, 5, 5),
)


def kernel(
    tokens, depth, classes, count_all,
    acts, probes, labels,
    grads, loss,
    a, w, at, acc, resid, lab, raw,
    snd, own, r2, xa2, xa1, za, zb4, zb, xb,
    l1, l2, l3, gauge, row_gauge,
    load_sem, label_sem, pair_send, pair_recv, send_sem, recv_sem, loss_send, loss_recv,
):
    dp = lax.axis_index("dp")
    core = lax.rem(dp, NC)
    chip = lax.div(dp, NC)
    x = lax.rem(chip, NX)
    z = lax.div(chip, NX)
    mate = 1 - core

    def at_x(step):
        return lax.rem(x + step + NX, NX)

    def at_z(step):
        return lax.rem(z + step + NZ, NZ)

    def device(zz, xx, cc):
        return {"dp": (zz * NX + xx) * NC + cc}

    pair = device(z, x, mate)
    along_x = [device(z, at_x(step), core) for step in range(1, NX)]
    along_z = [device(at_z(step), x, core) for step in range(1, NZ)]

    barrier = pltpu.get_barrier_semaphore()
    for peer in [pair] + along_x + along_z:
        pl.semaphore_signal(barrier, inc=1, device_id=peer, device_id_type=MESH)

    steps = depth // KSTEP
    tiles = KSTEP // TILE

    def loads(k):
        columns = pl.ds(pl.multiple_of(k * KSTEP, KSTEP), KSTEP)
        return (
            pltpu.make_async_copy(probes.at[0, columns, :], w.at[k], load_sem.at[0, k]),
            pltpu.make_async_copy(acts.at[0, :, columns], a.at[k], load_sem.at[1, k]),
        )

    for k in range(AHEAD):
        for load in loads(k):
            load.start()
    label_load = pltpu.make_async_copy(labels, raw, label_sem)
    label_load.start()

    acc[...] = jnp.zeros_like(acc)

    @pl.loop(0, steps)
    def _(k):
        for load in loads(k):
            load.wait()

        @pl.when(k + AHEAD < steps)
        def _():
            for load in loads(k + AHEAD):
                load.start()

        block = a[k]
        acc[...] += jnp.dot(block, w[k], preferred_element_type=F32)
        at[pl.ds(k * tiles, tiles)] = block.T.reshape(tiles, TILE, tokens)

    label_load.wait()
    for block in range(tokens // 128):
        row = jnp.broadcast_to(raw[block : block + 1, :], (128, 128))
        lab[block * 128 : (block + 1) * 128, :] = row.T
    part = jnp.zeros((8, 128), F32)
    lane = lax.broadcasted_iota(jnp.int32, (128, 128), 1)
    names = lax.broadcasted_iota(jnp.int32, (128, classes), 1)
    for block in range(tokens // 128):
        rows = slice(block * 128, (block + 1) * 128)
        logits = acc[rows, :]
        hit = jnp.concatenate([lab[rows, :]] * (classes // 128), axis=1) == names
        top = jnp.max(logits, axis=1, keepdims=True)
        expo = jnp.exp(logits - top)
        total = jnp.sum(expo, axis=1, keepdims=True)
        lse = top + jnp.log(total)
        probs = expo * (1.0 / total)
        resid[rows, :] = jnp.where(hit, probs - 1.0, probs).astype(BF16)
        picked = jnp.where(hit, logits, 0.0)
        picked = sum(picked[:, 128 * i : 128 * (i + 1)] for i in range(classes // 128))
        each = jnp.where(lane == 0, lse, 0.0) - picked
        part = part + jnp.sum(each.reshape(16, 8, 128), axis=0)
    l1[core] = jnp.sum(part, axis=0, keepdims=True)

    pl.semaphore_wait(barrier, NC + NX + NZ - 3)

    def whole_of(buf, count, sent_sem, got_sem):
        part = buf.at[pl.ds(0, count)]
        return pltpu.make_async_remote_copy(
            src_ref=part, dst_ref=part, send_sem=sent_sem, recv_sem=got_sem,
            device_id=pair, device_id_type=MESH,
        )

    def loss_copy(buf, mine, stage_index, to):
        return pltpu.make_async_remote_copy(
            src_ref=buf.at[mine], dst_ref=buf.at[mine],
            send_sem=loss_send, recv_sem=loss_recv.at[stage_index],
            device_id=to, device_id_type=MESH,
        )

    loss_stages = [
        [loss_copy(l1, core, 0, pair)],
        [loss_copy(l2, x, 1, to) for to in along_x],
        [loss_copy(l3, z, 2, to) for to in along_z],
    ]

    def loss_stage(step):
        if step > 0:
            whole_of(row_gauge, len(loss_stages[step - 1]), loss_send, loss_recv.at[step - 1]).wait_recv()
            if step == 1:
                l2[x] = l1[0] + l1[1]
            elif step == 2:
                l3[z] = (l2[0] + l2[1]) + (l2[2] + l2[3])
            else:
                rows = [l3[i] for i in range(NZ)]
                while len(rows) > 1:
                    rows = [p + q for p, q in zip(rows[::2], rows[1::2])]
                whole = jnp.sum(rows[0], axis=1, keepdims=True) / F32(count_all)
                loss[...] = jnp.broadcast_to(whole, (1, 128))
        if step < 3:
            for copy in loss_stages[step]:
                copy.start()

    def terms(tile):
        lhs = jnp.concatenate([at[i * 9 + tile] for i in range(NX * NZ)], axis=0)
        out = jnp.dot(lhs, resid[...], preferred_element_type=F32)
        return out.reshape(NX * NZ, 2, ROWS, classes)

    def store(buf, chunk, value):
        buf[chunk] = value.reshape(NZ, NX, ROWS, classes)

    def pair_copy(i):
        return pltpu.make_async_remote_copy(
            src_ref=snd.at[i], dst_ref=r2.at[i],
            send_sem=pair_send, recv_sem=pair_recv.at[i],
            device_id=pair, device_id_type=MESH,
        )

    pair_copies = [pair_copy(i) for i in range(9)]

    def terms_for_pair(k):
        both = terms(k + 5 * mate)
        for half in range(2):
            store(snd, 2 * k + half, both[:, half])
            pair_copies[2 * k + half].start()

    def terms_for_own(k):
        both = terms(k + 5 * core)
        for half in range(2):
            store(own, 2 * k + half, both[:, half])

    def terms_for_both():
        both = terms(4)
        first = core == 0
        store(snd, 8, jnp.where(first, both[:, 1], both[:, 0]))
        pair_copies[8].start()
        store(own, 8, jnp.where(first, both[:, 0], both[:, 1]))

    ring = {"x": (at_x, along_x, NX), "z": (at_z, along_z, NZ)}
    counts = []

    def size(i, stream, which, j):
        lanes = (WIDTHS[i] if stream == 0 else classes - WIDTHS[i]) // 128
        if which == 1:
            return lanes
        lanes *= NZ if stream == 0 else NX
        return lanes // 2 if j == (NX if stream == 0 else NZ) // 2 else lanes

    def slot(stream, step):
        return stream * MOST + step

    def parts(i, stream):
        wa = WIDTHS[i]
        plan = PLANS[i]
        if stream == 0:
            cols = pl.ds(0, wa)
            half = {1: pl.ds(0, NZ // 2), -1: pl.ds(NZ // 2, NZ // 2)}

            def first(j, d):
                if j == NX // 2:
                    side = (half[d], at_x(j * d), slice(None), cols)
                else:
                    side = (slice(None), at_x(j * d), slice(None), cols)
                return (i,) + side

            def first_land(j, d):
                if j == NX // 2:
                    return xa2, (i, SIDE[d], slice(None), slice(None), cols)
                return xa1, (i, SIDE[d], slice(None), slice(None), cols)

            def after(j, d, k):
                kept = half[d] if j == NX // 2 else slice(None)
                return (i, kept, at_x(k * d), slice(None), cols)

            def second(j, d):
                return (i, at_z(j * d), x, slice(None), cols)

            def second_land(j, d):
                return za, (i, j - 1, SIDE[d], slice(None), cols)

            return ("x", plan[0], first, first_land, after), ("z", plan[1], second, second_land, None)
        cols = pl.ds(wa, classes - wa)
        half = {1: pl.ds(0, NX // 2), -1: pl.ds(NX // 2, NX // 2)}

        def first(j, d):
            kept = half[d] if j == NZ // 2 else slice(None)
            return (i, at_z(j * d), kept, slice(None), cols)

        def first_land(j, d):
            if j == NZ // 2:
                return zb4, (i, SIDE[d], slice(None), slice(None), cols)
            return zb, (i, j - 1, SIDE[d], slice(None), slice(None), cols)

        def after(j, d, k):
            kept = half[d] if j == NZ // 2 else slice(None)
            return (i, at_z(k * d), kept, slice(None), cols)

        def second(j, d):
            return (i, z, at_x(j * d), slice(None), cols)

        def second_land(j, d):
            return xb, (i, j - 1, SIDE[d], slice(None), cols)

        return ("z", plan[2], first, first_land, after), ("x", plan[3], second, second_land, None)

    def moves(i, phase, big):
        far = 1 if i % 2 == 0 else -1
        axis, steps = phase[0], STEPS[phase[1]]
        top = ring[axis][2] // 2
        return [
            [(j, h, d) for j, h in step for d in (1, -1) if big or j < top or d == far]
            for step in steps
        ]

    def stage(i, stream, step):
        phases = parts(i, stream)
        todo = [(0, m) for m in moves(i, phases[0], True)] + [(1, m) for m in moves(i, phases[1], False)]
        if step == 0 and ready.setdefault(i, True):
            pair_copies[i].wait_recv()
            own[i] += r2[i]
            ready[i] = False
        if step > 0:
            which, group = todo[step - 1]
            axis, _, place, land, after = phases[which]
            finals = []
            count = sum(size(i, stream, which, j) for j, h, d in group)
            whole_of(gauge, count, send_sem, recv_sem.at[i, slot(stream, step - 1)]).wait_recv()
            for j, h, d in group:
                buf, index = land(j, d)
                if j == h:
                    finals.append((buf, index, j, d))
                else:
                    spot = after(j, d, j - h) if after else place(j - h, d)
                    own[spot] += buf[index]
            last.setdefault((i, stream, which), []).extend(finals)
            if step == len(todo) or todo[step][0] != which:
                finals = last[i, stream, which]
                top = ring[axis][2] // 2
                if which == 0:
                    whole = [buf[index] for buf, index, j, d in finals if j < top]
                    spot = place(0, 1)
                    total = own[spot]
                    for value in whole:
                        total += value
                    own[spot] = total
                    for buf, index, j, d in finals:
                        if j == top:
                            own[after(j, d, 0)] += buf[index]
                else:
                    total = own[place(0, 1)]
                    for buf, index, j, d in finals:
                        total += buf[index]
                    row = i * ROWS + core * ROWS if i < 8 else mate * (8 * ROWS)
                    rows = pl.ds(pl.multiple_of(row, ROWS), ROWS)
                    grads[rows, index[-1]] = total * F32(1.0 / count_all**0.5)
        if step < len(todo):
            which, group = todo[step]
            axis, _, place, land, _ = phases[which]
            _, peers, _ = ring[axis]
            for j, h, d in group:
                buf, index = land(j, d)
                copy = pltpu.make_async_remote_copy(
                    src_ref=own.at[place(j, d)], dst_ref=buf.at[index],
                    send_sem=send_sem, recv_sem=recv_sem.at[i, slot(stream, step)],
                    device_id=peers[h - 1 if d > 0 else len(peers) - h], device_id_type=MESH,
                )
                copy.start()
                counts.append(size(i, stream, which, j))

    SIDE = {1: 0, -1: 1}
    ready, last = {}, {}
    for code, i, step in ORDER:
        if code == 0:
            terms_for_pair(i)
        elif code == 1:
            terms_for_own(i)
        elif code == 2:
            terms_for_both()
        elif code == 5:
            loss_stage(step)
        else:
            stage(i, code - 3, step)

    pltpu.make_async_remote_copy(
        src_ref=snd, dst_ref=r2, send_sem=pair_send, recv_sem=pair_recv.at[0],
        device_id=pair, device_id_type=MESH,
    ).wait_send()
    whole_of(row_gauge, sum(len(group) for group in loss_stages), loss_send, loss_recv.at[0]).wait_send()
    assert sum(counts) == copied_tiles(classes)
    whole_of(gauge, sum(counts), send_sem, recv_sem.at[0, 0]).wait_send()


def copied_tiles(classes):
    total = 0
    for width, plan in zip(WIDTHS, PLANS):
        for lanes, first, second, n, m in (
            (width // 128, plan[0], plan[1], NX, NZ),
            ((classes - width) // 128, plan[2], plan[3], NZ, NX),
        ):
            for steps in STEPS[first]:
                total += sum(lanes * m * (1 if j == n // 2 else 2) for j, h in steps)
            for steps in STEPS[second]:
                total += sum(lanes * (1 if j == m // 2 else 2) for j, h in steps)
    return total


MOST = 6


def per_device(acts, probes, labels):
    tokens, depth = acts.shape[1:]
    classes = probes.shape[2]
    count_all = tokens * SHARDS
    n = depth // SHARDS // ROWS
    steps = depth // KSTEP
    vmem, sems = pltpu.VMEM, pltpu.SemaphoreType.DMA
    grads, loss = pl.pallas_call(
        lambda *refs: kernel(tokens, depth, classes, count_all, *refs),
        out_shape=(
            jax.ShapeDtypeStruct((depth // SHARDS, classes), F32),
            jax.ShapeDtypeStruct((1, 128), F32),
        ),
        in_specs=[
            pl.BlockSpec(memory_space=pl.ANY),
            pl.BlockSpec(memory_space=pl.ANY),
            pl.BlockSpec(memory_space=pl.ANY),
        ],
        out_specs=(pl.BlockSpec(memory_space=pltpu.VMEM),) * 2,
        scratch_shapes=[
            vmem((steps, tokens, KSTEP), BF16),
            vmem((steps, KSTEP, classes), BF16),
            vmem((depth // TILE, TILE, tokens), BF16),
            vmem((tokens, classes), F32),
            vmem((tokens, classes), BF16),
            vmem((tokens, 128), jnp.int32),
            vmem((tokens // 128, 128), jnp.int32),
            vmem((n, NZ, NX, ROWS, classes), F32),
            vmem((n, NZ, NX, ROWS, classes), F32),
            vmem((n, NZ, NX, ROWS, classes), F32),
            vmem((n, 2, NZ // 2, ROWS, classes), F32),
            vmem((n, 2, NZ, ROWS, classes), F32),
            vmem((n, 4, 2, ROWS, classes), F32),
            vmem((n, 2, NX // 2, ROWS, classes), F32),
            vmem((n, 3, 2, NX, ROWS, classes), F32),
            vmem((n, 2, 2, ROWS, classes), F32),
            vmem((NC, 1, 128), F32),
            vmem((NX, 1, 128), F32),
            vmem((NZ, 1, 128), F32),
            vmem((copied_tiles(classes), 8, 128), F32),
            vmem((16, 1, 128), F32),
            sems((2, steps)),
            sems(()),
            sems(()),
            sems((n,)),
            sems(()),
            sems((n, 2 * MOST)),
            sems(()),
            sems((3,)),
        ],
        compiler_params=pltpu.CompilerParams(
            collective_id=0, has_side_effects=True, vmem_limit_bytes=62 * 1024 * 1024
        ),
        name="probe_step",
    )(acts, probes, labels.reshape(tokens // 128, 128))
    return grads[None], loss[0, :1]


def solution(mesh):
    return jax.shard_map(
        per_device,
        mesh=mesh,
        in_specs=(P("layer", "dp", None), P("layer", None, None), P("dp")),
        out_specs=(P("layer", "dp", None), P("layer")),
        check_vma=False,
    )
```

```python
import jax
import jax.numpy as jnp
from jax import lax
from jax.experimental import pallas as pl
from jax.experimental.pallas import tpu as pltpu
from jax.sharding import PartitionSpec as P

F32 = jnp.float32
BF16 = jnp.bfloat16
MESH = pl.DeviceIdType.MESH

NX, NZ, NC = 4, 8, 2
SHARDS = NX * NZ * NC
ROWS = 8
TILE = 16
KSTEP = 768
AHEAD = 2

GROUPS = ((0, 1), (1, 1), (2, 2), (4, 2), (6, 2), (8, 1))
WIDTHS = (384, 128, 256, 384, 256, 384)
STEPS = {
    "x1": [[(2, 2), (1, 1)]],
    "x2": [[(2, 1)], [(1, 1)]],
    "z2": [[(4, 2), (3, 1)], [(2, 2), (1, 1)]],
    "z3": [[(4, 2), (3, 1)], [(2, 1)], [(1, 1)]],
    "z4": [[(4, 1)], [(3, 1)], [(2, 1)], [(1, 1)]],
}
PLANS = (
    ("x2", "z4", "z3", "x1"),
    ("x1", "z3", "z3", "x2"),
    ("x2", "z4", "z4", "x1"),
    ("x2", "z3", "z3", "x2"),
    ("x2", "z2", "z4", "x1"),
    ("x2", "z2", "z4", "x1"),
)
ORDER = (
    (0, 0, 0), (1, 0, 0), (0, 1, 0), (1, 1, 0), (5, 0, 0), (0, 2, 0), (3, 0, 0), (4, 0, 0),
    (1, 2, 0), (3, 1, 0), (4, 1, 0), (0, 3, 0), (1, 3, 0), (2, 0, 0), (3, 2, 0), (5, 0, 1),
    (4, 2, 0), (4, 0, 1), (3, 0, 1), (3, 3, 0), (4, 3, 0), (3, 1, 1), (4, 1, 1), (3, 4, 0),
    (4, 4, 0), (4, 2, 1), (3, 2, 1), (3, 5, 0), (4, 5, 0), (4, 0, 2), (4, 3, 1), (5, 0, 2),
    (3, 0, 2), (3, 1, 2), (4, 1, 2), (4, 4, 1), (3, 3, 1), (4, 2, 2), (3, 4, 1), (4, 5, 1),
    (4, 0, 3), (4, 3, 2), (3, 0, 3), (3, 1, 3), (4, 1, 3), (3, 2, 2), (5, 0, 3), (3, 5, 1),
    (4, 4, 2), (4, 2, 3), (4, 5, 2), (4, 3, 3), (3, 0, 4), (3, 1, 4), (3, 2, 3), (3, 3, 2),
    (4, 4, 3), (4, 2, 4), (3, 4, 2), (4, 5, 3), (3, 0, 5), (4, 1, 4), (3, 2, 4), (4, 0, 4),
    (3, 3, 3), (3, 5, 2), (4, 3, 4), (4, 4, 4), (4, 2, 5), (3, 4, 3), (4, 1, 5), (4, 5, 4),
    (3, 0, 6), (3, 2, 5), (3, 3, 4), (4, 3, 5), (3, 5, 3), (4, 4, 5), (3, 4, 4), (4, 5, 5),
    (3, 2, 6), (3, 3, 5), (3, 5, 4),
)


def kernel(
    tokens, depth, classes, count_all,
    acts, probes, labels,
    grads, loss,
    a, w, at, acc, resid, lab, raw,
    snd, own, r2, xa2, xa1, za, zb4, zb, xb,
    l1, l2, l3, gauge, row_gauge,
    load_sem, label_sem, pair_send, pair_recv, send_sem, recv_sem, loss_send, loss_recv,
):
    dp = lax.axis_index("dp")
    core = lax.rem(dp, NC)
    chip = lax.div(dp, NC)
    x = lax.rem(chip, NX)
    z = lax.div(chip, NX)
    mate = 1 - core

    def at_x(step):
        return lax.rem(x + step + NX, NX)

    def at_z(step):
        return lax.rem(z + step + NZ, NZ)

    def device(zz, xx, cc):
        return {"dp": (zz * NX + xx) * NC + cc}

    pair = device(z, x, mate)
    along_x = [device(z, at_x(step), core) for step in range(1, NX)]
    along_z = [device(at_z(step), x, core) for step in range(1, NZ)]

    barrier = pltpu.get_barrier_semaphore()
    for peer in [pair] + along_x + along_z:
        pl.semaphore_signal(barrier, inc=1, device_id=peer, device_id_type=MESH)

    steps = depth // KSTEP
    tiles = KSTEP // TILE

    def loads(k):
        columns = pl.ds(pl.multiple_of(k * KSTEP, KSTEP), KSTEP)
        return (
            pltpu.make_async_copy(probes.at[0, columns, :], w.at[k], load_sem.at[0, k]),
            pltpu.make_async_copy(acts.at[0, :, columns], a.at[k], load_sem.at[1, k]),
        )

    for k in range(AHEAD):
        for load in loads(k):
            load.start()
    label_load = pltpu.make_async_copy(labels, raw, label_sem)
    label_load.start()

    acc[...] = jnp.zeros_like(acc)

    @pl.loop(0, steps)
    def _(k):
        for load in loads(k):
            load.wait()

        @pl.when(k + AHEAD < steps)
        def _():
            for load in loads(k + AHEAD):
                load.start()

        block = a[k]
        acc[...] += jnp.dot(block, w[k], preferred_element_type=F32)
        at[pl.ds(k * tiles, tiles)] = block.T.reshape(tiles, TILE, tokens)

    label_load.wait()
    for block in range(tokens // 128):
        row = jnp.broadcast_to(raw[block : block + 1, :], (128, 128))
        lab[block * 128 : (block + 1) * 128, :] = row.T
    part = jnp.zeros((8, 128), F32)
    lane = lax.broadcasted_iota(jnp.int32, (128, 128), 1)
    names = lax.broadcasted_iota(jnp.int32, (128, classes), 1)
    for block in range(tokens // 128):
        rows = slice(block * 128, (block + 1) * 128)
        logits = acc[rows, :]
        hit = jnp.concatenate([lab[rows, :]] * (classes // 128), axis=1) == names
        top = jnp.max(logits, axis=1, keepdims=True)
        expo = jnp.exp(logits - top)
        total = jnp.sum(expo, axis=1, keepdims=True)
        lse = top + jnp.log(total)
        probs = expo * (1.0 / total)
        resid[rows, :] = jnp.where(hit, probs - 1.0, probs).astype(BF16)
        picked = jnp.where(hit, logits, 0.0)
        picked = sum(picked[:, 128 * i : 128 * (i + 1)] for i in range(classes // 128))
        each = jnp.where(lane == 0, lse, 0.0) - picked
        part = part + jnp.sum(each.reshape(16, 8, 128), axis=0)
    l1[core] = jnp.sum(part, axis=0, keepdims=True)

    pl.semaphore_wait(barrier, NC + NX + NZ - 3)

    def whole_of(buf, count, sent_sem, got_sem):
        part = buf.at[pl.ds(0, count)]
        return pltpu.make_async_remote_copy(
            src_ref=part, dst_ref=part, send_sem=sent_sem, recv_sem=got_sem,
            device_id=pair, device_id_type=MESH,
        )

    def loss_copy(buf, mine, stage_index, to):
        return pltpu.make_async_remote_copy(
            src_ref=buf.at[mine], dst_ref=buf.at[mine],
            send_sem=loss_send, recv_sem=loss_recv.at[stage_index],
            device_id=to, device_id_type=MESH,
        )

    loss_stages = [
        [loss_copy(l1, core, 0, pair)],
        [loss_copy(l2, x, 1, to) for to in along_x],
        [loss_copy(l3, z, 2, to) for to in along_z],
    ]

    def loss_stage(step):
        if step > 0:
            whole_of(row_gauge, len(loss_stages[step - 1]), loss_send, loss_recv.at[step - 1]).wait_recv()
            if step == 1:
                l2[x] = l1[0] + l1[1]
            elif step == 2:
                l3[z] = (l2[0] + l2[1]) + (l2[2] + l2[3])
            else:
                rows = [l3[i] for i in range(NZ)]
                while len(rows) > 1:
                    rows = [p + q for p, q in zip(rows[::2], rows[1::2])]
                whole = jnp.sum(rows[0], axis=1, keepdims=True) / F32(count_all)
                loss[...] = jnp.broadcast_to(whole, (1, 128))
        if step < 3:
            for copy in loss_stages[step]:
                copy.start()

    def terms(tile):
        lhs = jnp.concatenate([at[i * 9 + tile] for i in range(NX * NZ)], axis=0)
        out = jnp.dot(lhs, resid[...], preferred_element_type=F32)
        return out.reshape(NX * NZ, 2, ROWS, classes)

    def store(buf, chunk, value):
        buf[chunk] = value.reshape(NZ, NX, ROWS, classes)

    def pair_copy(i):
        return pltpu.make_async_remote_copy(
            src_ref=snd.at[i], dst_ref=r2.at[i],
            send_sem=pair_send, recv_sem=pair_recv.at[i],
            device_id=pair, device_id_type=MESH,
        )

    pair_copies = [pair_copy(i) for i in range(9)]

    def terms_for_pair(k):
        both = terms(k + 5 * mate)
        for half in range(2):
            store(snd, 2 * k + half, both[:, half])
            pair_copies[2 * k + half].start()

    def terms_for_own(k):
        both = terms(k + 5 * core)
        for half in range(2):
            store(own, 2 * k + half, both[:, half])

    def terms_for_both():
        both = terms(4)
        first = core == 0
        store(snd, 8, jnp.where(first, both[:, 1], both[:, 0]))
        pair_copies[8].start()
        store(own, 8, jnp.where(first, both[:, 0], both[:, 1]))

    ring = {"x": (at_x, along_x, NX), "z": (at_z, along_z, NZ)}
    counts = []

    def size(i, stream, which, j):
        lanes = (WIDTHS[i] if stream == 0 else classes - WIDTHS[i]) // 128 * GROUPS[i][1]
        if which == 1:
            return lanes
        lanes *= NZ if stream == 0 else NX
        return lanes // 2 if j == (NX if stream == 0 else NZ) // 2 else lanes

    def slot(stream, step):
        return stream * MOST + step

    def parts(i, stream):
        span = pl.ds(*GROUPS[i])
        wa = WIDTHS[i]
        plan = PLANS[i]
        if stream == 0:
            cols = pl.ds(0, wa)
            half = {1: pl.ds(0, NZ // 2), -1: pl.ds(NZ // 2, NZ // 2)}

            def first(j, d):
                if j == NX // 2:
                    side = (half[d], at_x(j * d), slice(None), cols)
                else:
                    side = (slice(None), at_x(j * d), slice(None), cols)
                return (span,) + side

            def first_land(j, d):
                if j == NX // 2:
                    return xa2, (span, SIDE[d], slice(None), slice(None), cols)
                return xa1, (span, SIDE[d], slice(None), slice(None), cols)

            def after(j, d, k):
                kept = half[d] if j == NX // 2 else slice(None)
                return (span, kept, at_x(k * d), slice(None), cols)

            def second(j, d):
                return (span, at_z(j * d), x, slice(None), cols)

            def second_land(j, d):
                return za, (span, j - 1, SIDE[d], slice(None), cols)

            return ("x", plan[0], first, first_land, after), ("z", plan[1], second, second_land, None)
        cols = pl.ds(wa, classes - wa)
        half = {1: pl.ds(0, NX // 2), -1: pl.ds(NX // 2, NX // 2)}

        def first(j, d):
            kept = half[d] if j == NZ // 2 else slice(None)
            return (span, at_z(j * d), kept, slice(None), cols)

        def first_land(j, d):
            if j == NZ // 2:
                return zb4, (span, SIDE[d], slice(None), slice(None), cols)
            return zb, (span, j - 1, SIDE[d], slice(None), slice(None), cols)

        def after(j, d, k):
            kept = half[d] if j == NZ // 2 else slice(None)
            return (span, at_z(k * d), kept, slice(None), cols)

        def second(j, d):
            return (span, z, at_x(j * d), slice(None), cols)

        def second_land(j, d):
            return xb, (span, j - 1, SIDE[d], slice(None), cols)

        return ("z", plan[2], first, first_land, after), ("x", plan[3], second, second_land, None)

    def moves(i, phase, big):
        far = 1 if i % 2 == 0 else -1
        axis, steps = phase[0], STEPS[phase[1]]
        top = ring[axis][2] // 2
        return [
            [(j, h, d) for j, h in step for d in (1, -1) if big or j < top or d == far]
            for step in steps
        ]

    def stage(i, stream, step):
        phases = parts(i, stream)
        todo = [(0, m) for m in moves(i, phases[0], True)] + [(1, m) for m in moves(i, phases[1], False)]
        if step == 0 and ready.setdefault(i, True):
            for chunk in range(GROUPS[i][0], sum(GROUPS[i])):
                pair_copies[chunk].wait_recv()
                own[chunk] += r2[chunk]
            ready[i] = False
        if step > 0:
            which, group = todo[step - 1]
            axis, _, place, land, after = phases[which]
            finals = []
            count = sum(size(i, stream, which, j) for j, h, d in group)
            whole_of(gauge, count, send_sem, recv_sem.at[i, slot(stream, step - 1)]).wait_recv()
            for j, h, d in group:
                buf, index = land(j, d)
                if j == h:
                    finals.append((buf, index, j, d))
                else:
                    spot = after(j, d, j - h) if after else place(j - h, d)
                    own[spot] += buf[index]
            last.setdefault((i, stream, which), []).extend(finals)
            if step == len(todo) or todo[step][0] != which:
                finals = last[i, stream, which]
                top = ring[axis][2] // 2
                if which == 0:
                    whole = [buf[index] for buf, index, j, d in finals if j < top]
                    spot = place(0, 1)
                    total = own[spot]
                    for value in whole:
                        total += value
                    own[spot] = total
                    for buf, index, j, d in finals:
                        if j == top:
                            own[after(j, d, 0)] += buf[index]
                else:
                    total = own[place(0, 1)]
                    for buf, index, j, d in finals:
                        total += buf[index]
                    chunk, height = GROUPS[i][0], GROUPS[i][1] * ROWS
                    row = (chunk + core) * ROWS if chunk < 8 else mate * (8 * ROWS)
                    rows = pl.ds(pl.multiple_of(row, ROWS), height)
                    total = total.reshape(height, total.shape[-1])
                    grads[rows, index[-1]] = total * F32(1.0 / count_all**0.5)
        if step < len(todo):
            which, group = todo[step]
            axis, _, place, land, _ = phases[which]
            _, peers, _ = ring[axis]
            for j, h, d in group:
                buf, index = land(j, d)
                copy = pltpu.make_async_remote_copy(
                    src_ref=own.at[place(j, d)], dst_ref=buf.at[index],
                    send_sem=send_sem, recv_sem=recv_sem.at[i, slot(stream, step)],
                    device_id=peers[h - 1 if d > 0 else len(peers) - h], device_id_type=MESH,
                )
                copy.start()
                counts.append(size(i, stream, which, j))

    SIDE = {1: 0, -1: 1}
    ready, last = {}, {}
    for code, i, step in ORDER:
        if code == 0:
            terms_for_pair(i)
        elif code == 1:
            terms_for_own(i)
        elif code == 2:
            terms_for_both()
        elif code == 5:
            loss_stage(step)
        else:
            stage(i, code - 3, step)

    pltpu.make_async_remote_copy(
        src_ref=snd, dst_ref=r2, send_sem=pair_send, recv_sem=pair_recv.at[0],
        device_id=pair, device_id_type=MESH,
    ).wait_send()
    whole_of(row_gauge, sum(len(group) for group in loss_stages), loss_send, loss_recv.at[0]).wait_send()
    assert sum(counts) == copied_tiles(classes)
    whole_of(gauge, sum(counts), send_sem, recv_sem.at[0, 0]).wait_send()


def copied_tiles(classes):
    total = 0
    for (_, height), width, plan in zip(GROUPS, WIDTHS, PLANS):
        for lanes, first, second, n, m in (
            (width // 128 * height, plan[0], plan[1], NX, NZ),
            ((classes - width) // 128 * height, plan[2], plan[3], NZ, NX),
        ):
            for steps in STEPS[first]:
                total += sum(lanes * m * (1 if j == n // 2 else 2) for j, h in steps)
            for steps in STEPS[second]:
                total += sum(lanes * (1 if j == m // 2 else 2) for j, h in steps)
    return total


MOST = 6


def per_device(acts, probes, labels):
    tokens, depth = acts.shape[1:]
    classes = probes.shape[2]
    count_all = tokens * SHARDS
    n = depth // SHARDS // ROWS
    steps = depth // KSTEP
    vmem, sems = pltpu.VMEM, pltpu.SemaphoreType.DMA
    grads, loss = pl.pallas_call(
        lambda *refs: kernel(tokens, depth, classes, count_all, *refs),
        out_shape=(
            jax.ShapeDtypeStruct((depth // SHARDS, classes), F32),
            jax.ShapeDtypeStruct((1, 128), F32),
        ),
        in_specs=[
            pl.BlockSpec(memory_space=pl.ANY),
            pl.BlockSpec(memory_space=pl.ANY),
            pl.BlockSpec(memory_space=pl.ANY),
        ],
        out_specs=(pl.BlockSpec(memory_space=pltpu.VMEM),) * 2,
        scratch_shapes=[
            vmem((steps, tokens, KSTEP), BF16),
            vmem((steps, KSTEP, classes), BF16),
            vmem((depth // TILE, TILE, tokens), BF16),
            vmem((tokens, classes), F32),
            vmem((tokens, classes), BF16),
            vmem((tokens, 128), jnp.int32),
            vmem((tokens // 128, 128), jnp.int32),
            vmem((n, NZ, NX, ROWS, classes), F32),
            vmem((n, NZ, NX, ROWS, classes), F32),
            vmem((n, NZ, NX, ROWS, classes), F32),
            vmem((n, 2, NZ // 2, ROWS, classes), F32),
            vmem((n, 2, NZ, ROWS, classes), F32),
            vmem((n, 4, 2, ROWS, classes), F32),
            vmem((n, 2, NX // 2, ROWS, classes), F32),
            vmem((n, 3, 2, NX, ROWS, classes), F32),
            vmem((n, 2, 2, ROWS, classes), F32),
            vmem((NC, 1, 128), F32),
            vmem((NX, 1, 128), F32),
            vmem((NZ, 1, 128), F32),
            vmem((copied_tiles(classes), 8, 128), F32),
            vmem((16, 1, 128), F32),
            sems((2, steps)),
            sems(()),
            sems(()),
            sems((n,)),
            sems(()),
            sems((len(GROUPS), 2 * MOST)),
            sems(()),
            sems((3,)),
        ],
        compiler_params=pltpu.CompilerParams(
            collective_id=0, has_side_effects=True, vmem_limit_bytes=62 * 1024 * 1024
        ),
        name="probe_step",
    )(acts, probes, labels.reshape(tokens // 128, 128))
    return grads[None], loss[0, :1]


def solution(mesh):
    return jax.shard_map(
        per_device,
        mesh=mesh,
        in_specs=(P("layer", "dp", None), P("layer", None, None), P("dp")),
        out_specs=(P("layer", "dp", None), P("layer")),
        check_vma=False,
    )
```
